128 devices in a mesh: chan: 4 (over y), tm: 32 (over z, x, core).
Axes of the slice: x: 4, y: 4, z: 4, core: 2. Of those that a mesh axis runs over, the one named last changes fastest.
Arguments:
- strain: float32 [768, 524288], P('chan', 'tm'), may hold values from -6 to 6
Outputs:
- power: float32 [768, 8192], P('chan', 'tm')
- nyquist: float32 [768], P('chan')
- mean_power: float32 [8192], P('tm')
The draws below stay inside these ranges and needn't reach their ends.
All inputs are finite; a program needn't handle non-finite values.
Results may differ from the reference program's by a relative error of at most 0.00007.
Values sent between devices are 32-bit elements; how exact they have to be, the bound alone decides.
No kernel may reach another device: no remote copies, remote signals or barrier semaphores. Data moves between devices by JAX's collectives and lax.ppermute only.
A program may use at most 192 MiB of HBM per device.

```python
import jax
import jax.numpy as jnp
from jax import lax

SEG = 16384
HOP = 8192
BINS = 8192
CHANNELS = 768
SAMPLES = 524288
SEGMENTS = 63


def level_of(stream_key, extent, split, low, top_value):
    loudness = 1.0
    for dim, shards_of in split:
        draws = jax.random.uniform(jax.random.fold_in(jax.random.fold_in(stream_key, 6), dim), (shards_of,), jnp.float32, low / len(split), top_value / len(split))
        loudness = loudness * jnp.repeat(jnp.exp(draws), extent[dim] // shards_of).reshape((-1,) + (1,) * (len(extent) - 1 - dim))
    return loudness


def bell_draw(key, dims, spread, most, cuts=(), kind=jnp.bfloat16):
    drawn = jax.random.normal(key, dims, jnp.float32) * spread
    if len(cuts) > 0:
        drawn = level_of(key, dims, cuts, -0.22, 0.18) * drawn
    return jnp.clip(drawn, min=-most, max=most).astype(kind)


def setup_inputs(seed: int = 0) -> dict:
    keys = jax.random.split(jax.random.key(seed), 2)
    strain = bell_draw(keys[0], (CHANNELS, SAMPLES), 1.0, 6.0, ((0, 4), (1, 32)), jnp.float32)
    return dict(strain=strain)


def hann_window():
    sample_pos = jnp.arange(SEG, dtype=jnp.float32)
    return 0.5 - 0.5 * jnp.cos(2.0 * jnp.pi * sample_pos / SEG)


def reference(strain):
    window = hann_window()
    energy = jnp.sum(window * window)

    def one_channel(signal):
        blocks = signal.reshape(SEGMENTS + 1, HOP)
        pieces = jnp.concatenate([blocks[:-1], blocks[1:]], axis=1)
        centred = (pieces - jnp.mean(pieces, axis=1, keepdims=True)) * window
        spectrum = jnp.fft.rfft(centred, axis=1)
        return jnp.sum(jnp.real(spectrum) ** 2 + jnp.imag(spectrum) ** 2, axis=0)

    totals = lax.map(one_channel, strain)
    doubling = jnp.where(jnp.arange(BINS) == 0, 1.0, 2.0).astype(totals.dtype)
    power = totals[:, :BINS] * doubling / (SEGMENTS * energy)
    nyquist = totals[:, BINS] / (SEGMENTS * energy)
    mean_power = jnp.mean(power, axis=0)
    return power, nyquist, mean_power
```

```python
import functools

import jax
import jax.numpy as jnp
import numpy as np
from jax import lax
from jax.experimental import pallas as pl
from jax.experimental.pallas import tpu as pltpu
from jax.sharding import PartitionSpec as P

SEG = 16384
ROOT = 128
HALF = ROOT // 2
TILE = 8
LANES = 128
STEPS = 4


def split_bf16(table):
    high = table.astype(jnp.bfloat16)
    low = (table - high.astype(np.float64)).astype(jnp.bfloat16)
    return high, low


def dft_constants():
    n = np.arange(ROOT)
    angle = 2.0 * np.pi * ((n[:, None] * n[None, :]) % ROOT) / ROOT
    rows = np.arange(HALF)
    first = np.concatenate([np.cos(angle[:HALF]), -np.sin(angle[:HALF])], axis=0)
    first[HALF] = 1.0 - 2.0 * (n % 2)
    high, low = split_bf16(first)
    first_high = np.concatenate([high, high], axis=1)
    twist = 2.0 * np.pi * (rows[:, None] * n[None, :]) / SEG
    cos_twist = np.cos(twist)
    cos_imag = cos_twist.copy()
    cos_imag[0] = 0.0
    twiddle = np.stack([cos_twist, cos_imag, np.sin(twist)]).astype(np.float32)
    edge = np.pi * n / ROOT
    edge_twiddle = np.stack([np.cos(edge), -np.sin(edge)]).astype(np.float32)
    halves = []
    for core in range(2):
        columns = []
        for half in (core, 1 - core):
            for place in range(16):
                shard = 2 * place + half
                for k in (2 * shard, 2 * shard + 1):
                    columns += [k, ROOT - 1 - k]
        halves.append(columns)
    second = []
    for columns in halves:
        c = np.cos(angle[:, columns])
        s = np.sin(angle[:, columns])
        full = np.block([[c, -s], [s, c]])
        h, l = split_bf16(full)
        second.append(np.concatenate([h, h, l], axis=0))
    return first_high, low, twiddle, edge_twiddle, np.stack(second)


def window_tables():
    pos = jnp.arange(SEG, dtype=jnp.float32)
    window = 0.5 - 0.5 * jnp.cos(2.0 * jnp.pi * pos / SEG)
    energy = jnp.sum(window * window)
    plain = window.reshape(ROOT, LANES)
    swapped = jnp.concatenate([plain[HALF:], plain[:HALF]], axis=0)
    return jnp.stack([plain, swapped]), energy


def spectrum_kernel(
    tiles,
    step,
    meta,
    x_ref,
    left_ref,
    right_ref,
    plain_ref,
    window_ref,
    first_ref,
    first_low_ref,
    twiddle_ref,
    edge_ref,
    second_ref,
    edges_in_ref,
    own_ref,
    other_ref,
    edges_ref,
    halo,
    spec,
    corner,
    result,
):
    i = pl.program_id(0)
    is_right = i >= tiles
    core = meta[0]

    @pl.when(i < tiles)
    def _():
        halo[...] = left_ref[0]

    @pl.when(is_right)
    def _():
        halo[...] = right_ref[0]

    @pl.when(i == 0)
    def _():
        edges_ref[...] = edges_in_ref[...]

    own_start = jnp.where(is_right, 0, HALF * TILE)
    keep = jnp.where(is_right, meta[2], meta[1]).astype(jnp.float32)
    cos_real = twiddle_ref[0]
    cos_imag = twiddle_ref[1]
    sin_both = twiddle_ref[2]
    for pair in range(TILE // 2):
        for seg in range(2):
            highs = []
            lows = []
            for c in (2 * pair, 2 * pair + 1):
                if seg == 0:
                    piece = x_ref[0, pl.ds(c, ROOT, stride=TILE), :]
                    window = plain_ref[0]
                else:
                    own = x_ref[0, pl.ds(own_start + c, HALF, stride=TILE), :]
                    piece = jnp.concatenate([own, halo[pl.ds(c, HALF, stride=TILE), :]], axis=0)
                    window = window_ref[0]
                mean = jnp.sum(piece, keepdims=True) * (1.0 / SEG)
                centred = (piece - mean) * window
                high = centred.astype(jnp.bfloat16)
                highs.append(high)
                lows.append((centred - high.astype(jnp.float32)).astype(jnp.bfloat16))
            high = jnp.concatenate(highs, axis=1)
            low = jnp.concatenate(lows, axis=1)
            stage = jnp.dot(
                first_ref[...], jnp.concatenate([high, low], axis=0), preferred_element_type=jnp.float32
            ) + jnp.dot(first_low_ref[...], high, preferred_element_type=jnp.float32)
            for q in range(2):
                c = 2 * pair + q
                real = stage[:HALF, q * LANES : (q + 1) * LANES]
                imag = stage[HALF:, q * LANES : (q + 1) * LANES]
                corner[seg * TILE + c : seg * TILE + c + 1, :] = imag[0:1]
                row = (seg * TILE + c) * HALF
                turned = (real * cos_real + imag * sin_both, imag * cos_imag - real * sin_both)
                for part in range(2):
                    value = turned[part]
                    high = value.astype(jnp.bfloat16)
                    lanes = slice(part * LANES, (part + 1) * LANES)
                    lanes_low = slice((2 + part) * LANES, (3 + part) * LANES)
                    spec[row : row + HALF, lanes] = high
                    spec[row : row + HALF, lanes_low] = (value - high.astype(jnp.float32)).astype(jnp.bfloat16)
    rows = 2 * TILE * HALF
    for part in range(2):
        value = corner[...] * edge_ref[part : part + 1]
        high = value.astype(jnp.bfloat16)
        spec[rows : rows + 2 * TILE, part * LANES : (part + 1) * LANES] = high
        spec[rows : rows + 2 * TILE, (2 + part) * LANES : (3 + part) * LANES] = (
            value - high.astype(jnp.float32)
        ).astype(jnp.bfloat16)
    weight = second_ref[0]
    result[...] = jnp.dot(spec[...], weight[: 4 * LANES], preferred_element_type=jnp.float32) + jnp.dot(
        spec[:, : 2 * LANES], weight[4 * LANES :], preferred_element_type=jnp.float32
    )

    def power_of(start, size):
        real = result[start : start + size, :LANES]
        imag = result[start : start + size, LANES:]
        return real * real + imag * imag

    edge_power = power_of(rows, TILE) + keep * power_of(rows + TILE, TILE)
    row_id = lax.broadcasted_iota(jnp.int32, (HALF, LANES), 0)
    lane_id = lax.broadcasted_iota(jnp.int32, (HALF, LANES), 1)
    replaced = (row_id == 0) & (lane_id % 2 == 1)
    tile_lane = lax.broadcasted_iota(jnp.int32, (TILE, LANES), 1)
    tile_row = lax.broadcasted_iota(jnp.int32, (TILE, LANES), 0)
    edge_lane = HALF - 1 + HALF * (1 - core)
    edge_tile = jnp.zeros((TILE, LANES), jnp.float32)
    columns = []
    for pair in range(TILE // 2):
        blocks = []
        for q in range(2):
            c = 2 * pair + q
            total = power_of(c * HALF, HALF) + keep * power_of((TILE + c) * HALF, HALF)
            edge_tile = jnp.where(tile_row == c, total[0:1], edge_tile)
            blocks.append(jnp.where(replaced, edge_power[c : c + 1], total))
        columns.append(jnp.concatenate(blocks, axis=0).T)
    edge_value = jnp.sum(jnp.where(tile_lane == edge_lane, edge_tile, 0.0), axis=1, keepdims=True)
    tile_number = jnp.where(is_right, 12 + i - tiles, i) + tiles * step
    edges_ref[...] = jnp.where(tile_lane == tile_number, edge_value, edges_ref[...])
    lower = tile_row < 4
    for group in range(2):
        a, b = columns[2 * group], columns[2 * group + 1]
        for half in range(2):
            out = own_ref if half == 0 else other_ref
            for place in range(8):
                start = half * HALF + place * TILE
                va, vb = a[start : start + TILE], b[start : start + TILE]
                out[2 * place, group] = jnp.where(lower, va, pltpu.roll(vb, 4, 0))
                out[2 * place + 1, group] = jnp.where(lower, pltpu.roll(va, 4, 0), vb)


def spectrum(step, tiles, meta, x, left, right, windows, constants, edges):
    first_high, first_low, twiddle, edge_twiddle, second = constants
    groups = 4 * tiles

    def tile_of(i):
        return jnp.where(i >= tiles, 12 + i - tiles, i) + tiles * step

    whole = lambda shape: pl.BlockSpec(shape, lambda i, m: (0,) * len(shape))
    out_block = pl.BlockSpec((16, 2, TILE, LANES), lambda i, m: (0, i, 0, 0))
    out_type = jax.ShapeDtypeStruct((16, groups, TILE, LANES), jnp.float32)
    return pl.pallas_call(
        functools.partial(spectrum_kernel, tiles, step),
        grid_spec=pltpu.PrefetchScalarGridSpec(
            num_scalar_prefetch=1,
            grid=(2 * tiles,),
            in_specs=[
                pl.BlockSpec((1, ROOT * TILE, LANES), lambda i, m: (tile_of(i), 0, 0)),
                pl.BlockSpec((1, HALF * TILE, LANES), lambda i, m: (jnp.minimum(i, tiles - 1), 0, 0)),
                pl.BlockSpec((1, HALF * TILE, LANES), lambda i, m: (jnp.maximum(i - tiles, 0), 0, 0)),
                pl.BlockSpec((1, ROOT, LANES), lambda i, m: (0, 0, 0)),
                pl.BlockSpec((1, ROOT, LANES), lambda i, m: (jnp.where(i >= tiles, 1, 0), 0, 0)),
                whole((ROOT, 2 * LANES)),
                whole((ROOT, LANES)),
                whole((3, HALF, LANES)),
                whole((2, LANES)),
                pl.BlockSpec((1, 6 * LANES, 2 * LANES), lambda i, m: (m[0], 0, 0)),
                whole((TILE, LANES)),
            ],
            out_specs=[out_block, out_block, whole((TILE, LANES))],
            scratch_shapes=[
                pltpu.VMEM((HALF * TILE, LANES), jnp.float32),
                pltpu.VMEM((2 * TILE * (HALF + 1), 4 * LANES), jnp.bfloat16),
                pltpu.VMEM((2 * TILE, LANES), jnp.float32),
                pltpu.VMEM((2 * TILE * (HALF + 1), 2 * LANES), jnp.float32),
            ],
        ),
        out_shape=[out_type, out_type, jax.ShapeDtypeStruct((TILE, LANES), jnp.float32)],
        compiler_params=pltpu.CompilerParams(dimension_semantics=("arbitrary",)),
        name="spectrum",
    )(meta, x, left, right, windows, windows, first_high, first_low, twiddle, edge_twiddle, second, edges)


def pick_constant():
    table = np.zeros((2, 2 * LANES, LANES), np.float32)
    for q in range(2):
        for k in range(HALF):
            table[q, q * HALF + k, k] = 1.0
            table[q, LANES + q * HALF + k, ROOT - k if k else HALF] = 1.0
    return table


def finish_kernel(tiles, meta, scale_ref, pick_ref, edges_ref, *refs):
    parts, (power_ref, mean_ref, nyquist_ref, band, spread) = refs[:STEPS], refs[STEPS:]
    shard = meta[3]
    for step, part in enumerate(parts):
        for side in range(2):
            total = part[0, side * 2 * tiles : (side + 1) * 2 * tiles]
            for source in range(1, 16):
                total = total + part[source, side * 2 * tiles : (side + 1) * 2 * tiles]
            first = (side * 12 + tiles * step) * 2 * TILE
            band[first : first + 2 * tiles * TILE] = total.reshape(2 * tiles * TILE, LANES)
    scale = scale_ref[0]
    lane = lax.broadcasted_iota(jnp.int32, (1, LANES), 1)
    sums = []
    for k in range(2):
        count = band.shape[0] // 4
        lo = band[pl.ds(2 * k, count, stride=4), :]
        hi = band[pl.ds(2 * k + 1, count, stride=4), :]
        both = jnp.concatenate([lo, hi], axis=1)
        first = (lane == 0) & (shard == 0) & (k == 0)
        factor = jnp.where(first, scale, 2.0 * scale)
        total = jnp.zeros((1, LANES), jnp.float32)
        for q in range(2):
            value = (
                jnp.dot(both, pick_ref[q], preferred_element_type=jnp.float32, precision=lax.Precision.HIGHEST)
                * factor
            )
            spread[k, pl.ds(q, count, stride=2), :] = value
            total = total + jnp.sum(value, axis=0, keepdims=True)
        power_ref[:, k * LANES : (k + 1) * LANES] = spread[k]
        sums.append(total)
    mean_ref[...] = jnp.concatenate(sums, axis=1)
    total = edges_ref[0]
    for source in range(1, 16):
        total = total + edges_ref[source]
    nyquist_ref[...] = (total * scale).T[:24]


def finish(tiles, meta, scale, parts, edges, rows):
    vmem = pl.BlockSpec(memory_space=pltpu.VMEM)
    smem = pl.BlockSpec(memory_space=pltpu.SMEM)
    return pl.pallas_call(
        functools.partial(finish_kernel, tiles),
        in_specs=[smem, smem, vmem, vmem] + [vmem] * len(parts),
        out_specs=[vmem, vmem, vmem],
        out_shape=[
            jax.ShapeDtypeStruct((rows, 2 * LANES), jnp.float32),
            jax.ShapeDtypeStruct((1, 2 * LANES), jnp.float32),
            jax.ShapeDtypeStruct((24, TILE), jnp.float32),
        ],
        scratch_shapes=[
            pltpu.VMEM((rows * 2, LANES), jnp.float32),
            pltpu.VMEM((2, rows, LANES), jnp.float32),
        ],
        name="finish",
    )(meta, scale, pick_constant(), edges, *parts)


def per_device(strain):
    rows, width = strain.shape
    count = lax.axis_size("tm")
    me = lax.axis_index("tm")
    row_tiles = rows // TILE
    tiles = row_tiles // 2 // STEPS
    segments = width // (SEG // 2) * count - 1
    x = strain.reshape(row_tiles, TILE, ROOT, LANES).swapaxes(1, 2).reshape(row_tiles, ROOT * TILE, LANES)
    to_left = [(i + 1, i) for i in range(count - 1)]
    to_right = [(i, i + 1) for i in range(count - 1)]
    halos = []
    for step in range(STEPS):
        first = step * tiles
        left = lax.ppermute(x[first : first + tiles, : HALF * TILE], "tm", to_left)
        right = lax.ppermute(x[12 + first : 12 + first + tiles, HALF * TILE :], "tm", to_right)
        halos.append((left, right))
    windows, energy = window_tables()
    scale = (1.0 / (segments * energy)).reshape(1)
    core = me % 2
    meta = jnp.stack([core, (me < count - 1).astype(jnp.int32), (me > 0).astype(jnp.int32), me]).astype(jnp.int32)
    constants = dft_constants()
    swap = [(i, i ^ 1) for i in range(count)]
    places = [[2 * p + c for p in range(count // 2)] for c in range(2)]
    edges = jnp.zeros((TILE, LANES), jnp.float32)
    parts = []
    for step in range(STEPS):
        own, other, edges = spectrum(step, tiles, meta, x, *halos[step], windows, constants, edges)
        if step == STEPS - 1:
            wide = (16, 1, TILE, LANES)
            own = jnp.concatenate([own, jnp.broadcast_to(edges, wide)], axis=1)
            other = jnp.concatenate([other, jnp.broadcast_to(edges, wide)], axis=1)
        mine = own + lax.ppermute(other, "tm", swap)
        parts.append(lax.all_to_all(mine, "tm", 0, 0, axis_index_groups=places, tiled=True))
    all_edges = parts[-1][:, 4 * tiles]
    power, band_sum, nyquist = finish(tiles, meta, scale, parts, all_edges, rows)
    chans = lax.axis_size("chan")
    total = band_sum
    for shift in range(1, chans):
        total = total + lax.ppermute(band_sum, "chan", [(i, (i + shift) % chans) for i in range(chans)])
    mean_power = (total / (rows * chans)).reshape(-1)
    return power, nyquist.reshape(-1), mean_power


def solution(mesh):
    in_specs = (P("chan", "tm"),)
    out_specs = (P("chan", "tm"), P("chan"), P("tm"))
    return jax.shard_map(per_device, mesh=mesh, in_specs=in_specs, out_specs=out_specs, check_vma=False)
```

```python
import functools

import jax
import jax.numpy as jnp
import numpy as np
from jax import lax
from jax.experimental import pallas as pl
from jax.experimental.pallas import tpu as pltpu
from jax.sharding import PartitionSpec as P


SEG = 16384
ROOT = 128
HALF = ROOT // 2
TILE = 8
LANES = 128
STEPS = 3
SIDE = 12
PLACES = 32
SEGS = 4
COST = 1 << 22


def split_bf16(table):
    high = table.astype(jnp.bfloat16)
    low = (table - high.astype(np.float64)).astype(jnp.bfloat16)
    return high, low


def dft_constants():
    n = np.arange(ROOT)
    angle = 2.0 * np.pi * ((n[:, None] * n[None, :]) % ROOT) / ROOT
    rows = np.arange(HALF)
    first = np.concatenate([np.cos(angle[:HALF]), -np.sin(angle[:HALF])], axis=0)
    first[HALF] = 1.0 - 2.0 * (n % 2)
    high, low = split_bf16(first)
    first_high = np.concatenate([high, high], axis=1)
    twist = 2.0 * np.pi * (rows[:, None] * n[None, :]) / SEG
    cos_twist = np.cos(twist)
    cos_imag = cos_twist.copy()
    cos_imag[0] = 0.0
    twiddle = np.stack([cos_twist, cos_imag, np.sin(twist)]).astype(np.float32)
    edge = np.pi * n / ROOT
    edge_twiddle = np.stack([np.cos(edge), -np.sin(edge)]).astype(np.float32)
    columns = []
    for k in range(HALF):
        columns += [k, ROOT - 1 - k]
    c = np.cos(angle[:, columns])
    s = np.sin(angle[:, columns])
    high, low_second = split_bf16(np.block([[c, -s], [s, c]]))
    second = np.concatenate([high, high, low_second], axis=0)
    return first_high, low, twiddle, edge_twiddle, second


def window_table():
    pos = jnp.arange(SEG, dtype=jnp.float32)
    window = 0.5 - 0.5 * jnp.cos(2.0 * jnp.pi * pos / SEG)
    energy = jnp.sum(window * window)
    return window.reshape(ROOT, LANES), energy


def spectrum_kernel(
    tiles,
    first,
    last,
    meta,
    x_hbm,
    remote_hbm,
    halo_a_hbm,
    halo_b_hbm,
    window_ref,
    first_ref,
    first_low_ref,
    twiddle_ref,
    edge_ref,
    second_ref,
    edges_in_ref,
    out_ref,
    edges_ref,
    x_buf,
    means,
    spec,
    corner,
    result,
    sems,
):
    group = pl.program_id(0)
    core = meta[0]
    near = pl.multiple_of(HALF + ROOT * core, HALF)
    far = pl.multiple_of(HALF + ROOT * (1 - core), HALF)

    def loads(place, tile, halo_hbm, halo_tile, right):
        at = pl.multiple_of(right * (5 * HALF), HALF)
        out = []
        for c in range(TILE):
            out.append((x_hbm.at[core * SIDE + tile, :, c, 0, :], x_buf.at[place, c, pl.ds(near, ROOT), :]))
            out.append((remote_hbm.at[tile, :, c, 0, :], x_buf.at[place, c, pl.ds(far, ROOT), :]))
            out.append((halo_hbm.at[halo_tile, :, c, 0, :], x_buf.at[place, c, pl.ds(at, HALF), :]))
        return [
            pltpu.make_async_copy(src, dst, sems.at[place, k]) for k, (src, dst) in enumerate(out)
        ]

    @pl.when(group == 0)
    def _():
        for u in range(tiles):
            for copy in loads(u, first + u, halo_a_hbm, u, 1 - core):
                copy.start()
        for u in range(tiles):
            for copy in loads(tiles + u, SIDE // 2 + first + u, halo_b_hbm, u, core):
                copy.start()
        edges_ref[...] = edges_in_ref[...]

    right = jnp.where(group == 0, 1 - core, core)
    keep = jnp.where(right == 1, meta[1], meta[2]).astype(jnp.float32)
    base = group * tiles
    outer_at = pl.multiple_of(right * (5 * HALF), HALF)
    outer_start = pl.multiple_of(right * (4 * HALF), HALF)
    starts = (HALF, 2 * HALF, 3 * HALF, outer_start)

    def wait_for(u):
        for copy in loads(base + u, first + u, halo_a_hbm, u, right):
            copy.wait()

    def average(u):
        def part(c, at):
            return jnp.sum(x_buf[base + u, c, pl.ds(at, HALF), :].reshape(HALF // TILE, TILE, LANES), axis=0)

        sums = [[] for _ in range(SEGS)]
        for c in range(TILE):
            q = [part(c, HALF * (k + 1)) for k in range(4)]
            outer = part(c, outer_at) + jnp.where(right == 1, q[3], q[0])
            for k, value in enumerate((q[0] + q[1], q[1] + q[2], q[2] + q[3], outer)):
                sums[k].append(value)
        both = jnp.stack(sum(sums, []))
        total = jnp.sum(jnp.sum(both, axis=1), axis=1, keepdims=True) * (1.0 / SEG)
        means[u] = jnp.broadcast_to(total, (SEGS * TILE, LANES))

    def put(u, row, size, part, value):
        high = value.astype(jnp.bfloat16)
        lanes = slice(part * LANES, (part + 1) * LANES)
        lanes_low = slice((2 + part) * LANES, (3 + part) * LANES)
        spec[u, row : row + size, lanes] = high
        spec[u, row : row + size, lanes_low] = (value - high.astype(jnp.float32)).astype(jnp.bfloat16)

    def forward(u):
        for pair in range(TILE // 2):
            for seg in range(SEGS):
                highs = []
                lows = []
                for c in (2 * pair, 2 * pair + 1):
                    r = seg * TILE + c
                    piece = x_buf[base + u, c, pl.ds(starts[seg], ROOT), :]
                    centred = (piece - means[u, r : r + 1, :]) * window_ref[...]
                    high = centred.astype(jnp.bfloat16)
                    highs.append(high)
                    lows.append((centred - high.astype(jnp.float32)).astype(jnp.bfloat16))
                high = jnp.concatenate(highs, axis=1)
                low = jnp.concatenate(lows, axis=1)
                stage = jnp.dot(
                    first_ref[...], jnp.concatenate([high, low], axis=0), preferred_element_type=jnp.float32
                ) + jnp.dot(first_low_ref[...], high, preferred_element_type=jnp.float32)
                for q in range(2):
                    r = seg * TILE + 2 * pair + q
                    real = stage[:HALF, q * LANES : (q + 1) * LANES]
                    imag = stage[HALF:, q * LANES : (q + 1) * LANES]
                    corner[u, r : r + 1, :] = imag[0:1]
                    put(u, r * HALF, HALF, 0, real * twiddle_ref[0] + imag * twiddle_ref[2])
                    put(u, r * HALF, HALF, 1, imag * twiddle_ref[1] - real * twiddle_ref[2])

    rows = SEGS * TILE * HALF

    def second(u):
        for part in range(2):
            put(u, rows, SEGS * TILE, part, corner[u] * edge_ref[part : part + 1])
        result[u] = jnp.dot(
            spec[u], second_ref[: 4 * LANES, :], preferred_element_type=jnp.float32
        ) + jnp.dot(spec[u, :, : 2 * LANES], second_ref[4 * LANES :, :], preferred_element_type=jnp.float32)

    row_id = lax.broadcasted_iota(jnp.int32, (HALF, LANES), 0)
    lane_id = lax.broadcasted_iota(jnp.int32, (HALF, LANES), 1)
    replaced = (row_id == 0) & (lane_id % 2 == 1)
    tile_lane = lax.broadcasted_iota(jnp.int32, (TILE, LANES), 1)
    tile_row = lax.broadcasted_iota(jnp.int32, (TILE, LANES), 0)
    lower_rows = tile_row < TILE // 2

    def emit(u):
        def power_of(start, size):
            real = result[u, start : start + size, :LANES]
            imag = result[u, start : start + size, LANES:]
            return real * real + imag * imag

        def all_segments(start, step, size):
            inner = power_of(start, size) + power_of(start + step, size) + power_of(start + 2 * step, size)
            return inner + keep * power_of(start + 3 * step, size)

        edge_power = all_segments(rows, TILE, TILE)
        edge_tile = jnp.zeros((TILE, LANES), jnp.float32)
        columns = []
        for pair in range(TILE // 2):
            blocks = []
            for q in range(2):
                c = 2 * pair + q
                total = all_segments(c * HALF, TILE * HALF, HALF)
                edge_tile = jnp.where(tile_row == c, total[0:1], edge_tile)
                blocks.append(jnp.where(replaced, edge_power[c : c + 1], total))
            columns.append(jnp.concatenate(blocks, axis=0).T)
        edge_value = jnp.sum(jnp.where(tile_lane == LANES - 1, edge_tile, 0.0), axis=1, keepdims=True)
        tile_number = group * (SIDE // 2) + first + u
        edges_ref[...] = jnp.where(tile_lane == tile_number, edge_value, edges_ref[...])
        at = 2 * (base + u)
        for half in range(2):
            a, b = columns[2 * half], columns[2 * half + 1]
            for place in range(PLACES // 2):
                va = a[place * TILE : (place + 1) * TILE]
                vb = b[place * TILE : (place + 1) * TILE]
                out_ref[2 * place, at + half] = jnp.where(lower_rows, va, pltpu.roll(vb, 4, 0))
                out_ref[2 * place + 1, at + half] = jnp.where(lower_rows, pltpu.roll(va, 4, 0), vb)

    for u in range(tiles):
        wait_for(u)
    for u in range(tiles):
        average(u)
    for u in range(tiles):
        forward(u)
        second(u)
        if u > 0:
            emit(u - 1)
    emit(tiles - 1)
    if last:

        @pl.when(group == 1)
        def _():
            for place in range(PLACES):
                out_ref[place, 4 * tiles] = edges_ref[...]


def spectrum(first, tiles, last, meta, x, remote, halo_a, halo_b, window, constants, edges):
    first_high, first_low, twiddle, edge_twiddle, second = constants
    whole = lambda shape: pl.BlockSpec(shape, lambda i, m: (0,) * len(shape))
    hbm = pl.BlockSpec(memory_space=pl.ANY)
    out_shape = (PLACES, 4 * tiles + int(last), TILE, LANES)
    rows = SEGS * TILE * (HALF + 1)
    by_channel = lambda v: v.reshape(-1, v.shape[1] // TILE, TILE, 1, LANES)
    work = 2 * tiles * SEGS * TILE
    return pl.pallas_call(
        functools.partial(spectrum_kernel, tiles, first, last),
        grid_spec=pltpu.PrefetchScalarGridSpec(
            num_scalar_prefetch=1,
            grid=(2,),
            in_specs=[
                hbm,
                hbm,
                hbm,
                hbm,
                whole((ROOT, LANES)),
                whole((ROOT, 2 * LANES)),
                whole((ROOT, LANES)),
                whole((3, HALF, LANES)),
                whole((2, LANES)),
                whole((6 * LANES, 2 * LANES)),
                whole((TILE, LANES)),
            ],
            out_specs=[whole(out_shape), whole((TILE, LANES))],
            scratch_shapes=[
                pltpu.VMEM((2 * tiles, TILE, 6 * HALF, LANES), jnp.float32),
                pltpu.VMEM((tiles, SEGS * TILE, LANES), jnp.float32),
                pltpu.VMEM((tiles, rows, 4 * LANES), jnp.bfloat16),
                pltpu.VMEM((tiles, SEGS * TILE, LANES), jnp.float32),
                pltpu.VMEM((tiles, rows, 2 * LANES), jnp.float32),
                pltpu.SemaphoreType.DMA((2 * tiles, 3 * TILE)),
            ],
        ),
        out_shape=[
            jax.ShapeDtypeStruct(out_shape, jnp.float32),
            jax.ShapeDtypeStruct((TILE, LANES), jnp.float32),
        ],
        compiler_params=pltpu.CompilerParams(dimension_semantics=("arbitrary",)),
        cost_estimate=pl.CostEstimate(flops=work * COST, transcendentals=0, bytes_accessed=work * SEG * 4),
        name="spectrum",
    )(
        meta,
        by_channel(x),
        by_channel(remote),
        by_channel(halo_a),
        by_channel(halo_b),
        window,
        first_high,
        first_low,
        twiddle,
        edge_twiddle,
        second,
        edges,
    )


def pick_constant():
    table = np.zeros((2, 2 * LANES, LANES), np.float32)
    for q in range(2):
        for k in range(HALF):
            table[q, q * HALF + k, k] = 1.0
            table[q, LANES + q * HALF + k, ROOT - k if k else HALF] = 1.0
    return table


def finish_kernel(tiles, meta, scale_ref, pick_ref, *refs):
    parts, (power_ref, mean_ref, nyquist_ref, band, spread) = refs[:STEPS], refs[STEPS:]
    shard = meta[3]
    for step, part in enumerate(parts):
        for core in range(2):
            for group in range(2):
                span = slice(group * 2 * tiles, (group + 1) * 2 * tiles)
                total = part[core, span]
                for source in range(2 + core, PLACES, 2):
                    total = total + part[source, span]
                first = (core * SIDE + group * (SIDE // 2) + tiles * step) * 2 * TILE
                band[first : first + 2 * tiles * TILE] = total.reshape(2 * tiles * TILE, LANES)
    scale = scale_ref[0]
    lane = lax.broadcasted_iota(jnp.int32, (1, LANES), 1)
    sums = []
    for k in range(2):
        count = band.shape[0] // 4
        lo = band[pl.ds(2 * k, count, stride=4), :]
        hi = band[pl.ds(2 * k + 1, count, stride=4), :]
        both = jnp.concatenate([lo, hi], axis=1)
        first = (lane == 0) & (shard == 0) & (k == 0)
        factor = jnp.where(first, scale, 2.0 * scale)
        total = jnp.zeros((1, LANES), jnp.float32)
        for q in range(2):
            value = (
                jnp.dot(both, pick_ref[q], preferred_element_type=jnp.float32, precision=lax.Precision.HIGHEST)
                * factor
            )
            spread[k, pl.ds(q, count, stride=2), :] = value
            total = total + jnp.sum(value, axis=0, keepdims=True)
        power_ref[:, k * LANES : (k + 1) * LANES] = spread[k]
        sums.append(total)
    mean_ref[...] = jnp.concatenate(sums, axis=1)
    for core in range(2):
        total = parts[-1][core, 4 * tiles]
        for source in range(2 + core, PLACES, 2):
            total = total + parts[-1][source, 4 * tiles]
        nyquist_ref[core * SIDE : (core + 1) * SIDE] = (total * scale).T[:SIDE]


def finish(tiles, meta, scale, parts, rows):
    vmem = pl.BlockSpec(memory_space=pltpu.VMEM)
    smem = pl.BlockSpec(memory_space=pltpu.SMEM)
    return pl.pallas_call(
        functools.partial(finish_kernel, tiles),
        in_specs=[smem, smem, vmem] + [vmem] * len(parts),
        out_specs=[vmem, vmem, vmem],
        out_shape=[
            jax.ShapeDtypeStruct((rows, 2 * LANES), jnp.float32),
            jax.ShapeDtypeStruct((1, 2 * LANES), jnp.float32),
            jax.ShapeDtypeStruct((2 * SIDE, TILE), jnp.float32),
        ],
        scratch_shapes=[
            pltpu.VMEM((rows * 2, LANES), jnp.float32),
            pltpu.VMEM((2, rows, LANES), jnp.float32),
        ],
        name="finish",
    )(meta, scale, pick_constant(), *parts)


def per_device(strain):
    rows, width = strain.shape
    count = lax.axis_size("tm")
    me = lax.axis_index("tm")
    row_tiles = rows // TILE
    tiles = SIDE // 2 // STEPS
    segments = width // (SEG // 2) * count - 1
    core = me & 1
    x = strain.reshape(row_tiles, TILE, ROOT, LANES).swapaxes(1, 2).reshape(row_tiles, ROOT * TILE, LANES)
    same = [(i + 2, i) for i in range(0, count - 2, 2)] + [(i, i + 2) for i in range(1, count - 2, 2)]
    cross = [(i, i + 1) for i in range(1, count - 2, 2)] + [(i + 1, i) for i in range(1, count - 2, 2)]
    swap = [(i, i ^ 1) for i in range(count)]

    def part(tile, offset, tile_count, size):
        return lax.dynamic_slice(x, (tile, offset, 0), (tile_count, size, LANES))

    edge_at = core * (HALF * TILE)
    halos = []
    for step in range(STEPS):
        at = step * tiles
        halo_a = lax.ppermute(part(core * SIDE + at, edge_at, tiles, HALF * TILE), "tm", same)
        halo_b = lax.ppermute(
            part((1 - core) * SIDE + SIDE // 2 + at, edge_at, tiles, HALF * TILE), "tm", cross
        )
        halos.append((halo_a, halo_b))
    remote = lax.ppermute(part((1 - core) * SIDE, 0, SIDE, ROOT * TILE), "tm", swap)
    window, energy = window_table()
    scale = (1.0 / (segments * energy)).reshape(1)
    meta = jnp.stack([core, (me < count - 2).astype(jnp.int32), (me > 1).astype(jnp.int32), me]).astype(jnp.int32)
    constants = dft_constants()
    edges = jnp.zeros((TILE, LANES), jnp.float32)
    parts = []
    for step in range(STEPS):
        out, edges = spectrum(
            step * tiles, tiles, step == STEPS - 1, meta, x, remote, *halos[step], window, constants, edges
        )
        parts.append(lax.all_to_all(out, "tm", 0, 0, tiled=True))
    power, band_sum, nyquist = finish(tiles, meta, scale, parts, rows)
    chans = lax.axis_size("chan")
    total = band_sum
    for shift in range(1, chans):
        total = total + lax.ppermute(band_sum, "chan", [(i, (i + shift) % chans) for i in range(chans)])
    mean_power = (total / (rows * chans)).reshape(-1)
    return power, nyquist.reshape(-1), mean_power


def solution(mesh):
    in_specs = (P("chan", "tm"),)
    out_specs = (P("chan", "tm"), P("chan"), P("tm"))
    return jax.shard_map(per_device, mesh=mesh, in_specs=in_specs, out_specs=out_specs, check_vma=False)
```

```python
import functools

import jax
import jax.numpy as jnp
import numpy as np
from jax import lax
from jax.experimental import pallas as pl
from jax.experimental.pallas import tpu as pltpu
from jax.sharding import PartitionSpec as P


SEG = 16384
ROOT = 128
HALF = ROOT // 2
TILE = 8
LANES = 128
CHUNKS = (4, 8)
STEPS = len(CHUNKS)
SIDE = 12
PLACES = 32
SEGS = 4
COST = 1 << 22


def split_bf16(table):
    high = table.astype(jnp.bfloat16)
    low = (table - high.astype(np.float64)).astype(jnp.bfloat16)
    return high, low


def dft_constants():
    n = np.arange(ROOT)
    angle = 2.0 * np.pi * ((n[:, None] * n[None, :]) % ROOT) / ROOT
    rows = np.arange(HALF)
    first = np.concatenate([np.cos(angle[:HALF]), -np.sin(angle[:HALF])], axis=0)
    first[HALF] = 1.0 - 2.0 * (n % 2)
    high, low = split_bf16(first)
    first_high = np.concatenate([high, high], axis=1)
    twist = 2.0 * np.pi * (rows[:, None] * n[None, :]) / SEG
    cos_twist = np.cos(twist)
    cos_imag = cos_twist.copy()
    cos_imag[0] = 0.0
    twiddle = np.stack([cos_twist, cos_imag, np.sin(twist)]).astype(np.float32)
    edge = np.pi * n / ROOT
    edge_twiddle = np.stack([np.cos(edge), -np.sin(edge)]).astype(np.float32)
    columns = []
    for k in range(HALF):
        columns += [k, ROOT - 1 - k]
    c = np.cos(angle[:, columns])
    s = np.sin(angle[:, columns])
    high, low_second = split_bf16(np.block([[c, -s], [s, c]]))
    second = np.concatenate([high, high, low_second], axis=0)
    window = (0.5 - 0.5 * np.cos(2.0 * np.pi * np.arange(SEG) / SEG)).astype(np.float32)
    reals = np.concatenate([window.reshape(ROOT, LANES), *twiddle, edge_twiddle, np.zeros((6, LANES), np.float32)])
    left = np.concatenate([first_high, low], axis=1)
    return reals, left, second, float(np.sum(window.astype(np.float64) ** 2))


def spectrum_kernel(
    tiles,
    first,
    skip,
    last,
    x_hbm,
    remote_hbm,
    halo_hbm,
    reals_ref,
    first_ref,
    second_ref,
    edges_in_ref,
    out_ref,
    edges_ref,
    x_buf,
    means,
    spec,
    corner,
    result,
    sems,
):
    step = pl.program_id(0)
    me = lax.axis_index("tm")
    core = me & 1
    right = 1 - core
    near = pl.multiple_of(HALF + ROOT * core, HALF)
    far = pl.multiple_of(HALF + ROOT * right, HALF)
    outer_at = pl.multiple_of(right * (5 * HALF), HALF)
    outer_start = pl.multiple_of(right * (4 * HALF), HALF)
    starts = (HALF, 2 * HALF, 3 * HALF, outer_start)
    inside = jnp.where(right == 1, me < lax.axis_size("tm") - 2, me > 1)
    keep = jnp.where(inside, 1.0, 0.0).astype(jnp.float32)
    base = step

    @pl.when(step == 0)
    def _():
        for u in range(tiles):
            for c in range(TILE):
                for src, at, size in (
                    (x_hbm.at[core * SIDE + first + u, :, c, 0, :], near, ROOT),
                    (remote_hbm.at[skip + u, :, c, 0, :], far, ROOT),
                    (halo_hbm.at[skip + u, :, c, 0, :], outer_at, HALF),
                ):
                    pltpu.make_async_copy(src, x_buf.at[u, c, pl.ds(at, size), :], sems.at[u]).start()
        edges_ref[...] = edges_in_ref[...] if first else jnp.zeros((TILE, LANES), jnp.float32)

    def wait_for(u):
        whole = x_buf.at[base + u, :, pl.ds(0, 5 * HALF), :]
        pltpu.make_async_copy(whole, whole, sems.at[base + u]).wait()

    def average(u):
        def part(c, at):
            return jnp.sum(x_buf[base + u, c, pl.ds(at, HALF), :].reshape(HALF // TILE, TILE, LANES), axis=0)

        sums = [[] for _ in range(SEGS)]
        for c in range(TILE):
            q = [part(c, HALF * (k + 1)) for k in range(4)]
            outer = part(c, outer_at) + jnp.where(right == 1, q[3], q[0])
            for k, value in enumerate((q[0] + q[1], q[1] + q[2], q[2] + q[3], outer)):
                sums[k].append(value)
        both = jnp.stack(sum(sums, []))
        total = jnp.sum(jnp.sum(both, axis=1), axis=1, keepdims=True) * (1.0 / SEG)
        means[...] = jnp.broadcast_to(total, (SEGS * TILE, LANES))

    def put(pair, row, size, part, value):
        high = value.astype(jnp.bfloat16)
        lanes = slice(part * LANES, (part + 1) * LANES)
        lanes_low = slice((2 + part) * LANES, (3 + part) * LANES)
        spec[pair, row : row + size, lanes] = high
        spec[pair, row : row + size, lanes_low] = (value - high.astype(jnp.float32)).astype(jnp.bfloat16)

    rows = 2 * SEGS * HALF

    def forward(pair):
        for seg in range(SEGS):
            highs = []
            lows = []
            for q in range(2):
                c = 2 * pair + q
                r = seg * TILE + c
                piece = x_buf[step, c, pl.ds(starts[seg], ROOT), :]
                centred = (piece - means[r : r + 1, :]) * reals_ref[:ROOT]
                high = centred.astype(jnp.bfloat16)
                highs.append(high)
                lows.append((centred - high.astype(jnp.float32)).astype(jnp.bfloat16))
            high = jnp.concatenate(highs, axis=1)
            low = jnp.concatenate(lows, axis=1)
            stage = jnp.dot(
                first_ref[...], jnp.concatenate([high, low, high], axis=0), preferred_element_type=jnp.float32
            )
            for q in range(2):
                real = stage[:HALF, q * LANES : (q + 1) * LANES]
                imag = stage[HALF:, q * LANES : (q + 1) * LANES]
                r = 2 * seg + q
                corner[pair, r : r + 1, :] = imag[0:1]
                cos_real = reals_ref[ROOT : ROOT + HALF]
                cos_imag = reals_ref[ROOT + HALF : 2 * ROOT]
                sin_both = reals_ref[2 * ROOT : 2 * ROOT + HALF]
                put(pair, r * HALF, HALF, 0, real * cos_real + imag * sin_both)
                put(pair, r * HALF, HALF, 1, imag * cos_imag - real * sin_both)

    def second(pair):
        edge = 2 * ROOT + HALF
        for part in range(2):
            put(pair, rows, TILE, part, corner[pair] * reals_ref[edge + part : edge + part + 1])
        left = jnp.concatenate([spec[pair], spec[pair, :, : 2 * LANES]], axis=1)
        result[pair] = jnp.dot(left, second_ref[...], preferred_element_type=jnp.float32)

    row_id = lax.broadcasted_iota(jnp.int32, (HALF, LANES), 0)
    lane_id = lax.broadcasted_iota(jnp.int32, (HALF, LANES), 1)
    replaced = (row_id == 0) & (lane_id % 2 == 1)
    tile_lane = lax.broadcasted_iota(jnp.int32, (TILE, LANES), 1)
    tile_row = lax.broadcasted_iota(jnp.int32, (TILE, LANES), 0)
    lower_rows = tile_row < TILE // 2
    edge_rows = []

    def column(pair):
        def power_of(start, size):
            real = result[pair, start : start + size, :LANES]
            imag = result[pair, start : start + size, LANES:]
            return real * real + imag * imag

        edge_power = power_of(rows, TILE)
        blocks = []
        for q in range(2):
            total = keep * power_of((6 + q) * HALF, HALF)
            edge = keep * edge_power[6 + q : 7 + q]
            for seg in range(3):
                total = total + power_of((2 * seg + q) * HALF, HALF)
                edge = edge + edge_power[2 * seg + q : 2 * seg + q + 1]
            edge_rows.append(total[0:1])
            blocks.append(jnp.where(replaced, edge, total))
        return jnp.concatenate(blocks, axis=0).T

    def store(half, a, b):
        at = 2 * step + half
        for place in range(PLACES // 2):
            va = a[place * TILE : (place + 1) * TILE]
            vb = b[place * TILE : (place + 1) * TILE]
            out_ref[2 * place, at] = jnp.where(lower_rows, va, pltpu.roll(vb, 4, 0))
            out_ref[2 * place + 1, at] = jnp.where(lower_rows, pltpu.roll(va, 4, 0), vb)

    wait_for(0)
    average(0)
    forward(0)
    second(0)
    forward(1)
    second(1)
    first_column = column(0)
    forward(2)
    second(2)
    store(0, first_column, column(1))
    forward(3)
    second(3)
    first_column = column(2)
    store(1, first_column, column(3))
    edge_tile = jnp.zeros((TILE, LANES), jnp.float32)
    for c, row in enumerate(edge_rows):
        edge_tile = jnp.where(tile_row == c, row, edge_tile)
    edge_value = jnp.sum(jnp.where(tile_lane == LANES - 1, edge_tile, 0.0), axis=1, keepdims=True)
    edges_ref[...] = jnp.where(tile_lane == first + step, edge_value, edges_ref[...])
    if last:

        @pl.when(step == tiles - 1)
        def _():
            for place in range(PLACES):
                out_ref[place, 2 * tiles] = edges_ref[...]


def spectrum(first, tiles, skip, last, x, remote, halo, constants, edges):
    reals, left, second, _ = constants
    whole = lambda shape: pl.BlockSpec(shape, lambda i: (0,) * len(shape))
    hbm = pl.BlockSpec(memory_space=pl.ANY)
    out_shape = (PLACES, 2 * tiles + int(last), TILE, LANES)
    rows = 2 * SEGS * HALF + TILE
    by_channel = lambda v: v.reshape(-1, v.shape[1] // TILE, TILE, 1, LANES)
    work = tiles * SEGS * TILE
    return pl.pallas_call(
        functools.partial(spectrum_kernel, tiles, first, skip, last),
        grid_spec=pltpu.PrefetchScalarGridSpec(
            num_scalar_prefetch=0,
            grid=(tiles,),
            in_specs=[
                hbm,
                hbm,
                hbm,
                whole(reals.shape),
                whole(left.shape),
                whole(second.shape),
                whole((TILE, LANES)),
            ],
            out_specs=[whole(out_shape), whole((TILE, LANES))],
            scratch_shapes=[
                pltpu.VMEM((tiles, TILE, 6 * HALF, LANES), jnp.float32),
                pltpu.VMEM((SEGS * TILE, LANES), jnp.float32),
                pltpu.VMEM((TILE // 2, rows, 4 * LANES), jnp.bfloat16),
                pltpu.VMEM((TILE // 2, TILE, LANES), jnp.float32),
                pltpu.VMEM((TILE // 2, rows, 2 * LANES), jnp.float32),
                pltpu.SemaphoreType.DMA((tiles,)),
            ],
        ),
        out_shape=[
            jax.ShapeDtypeStruct(out_shape, jnp.float32),
            jax.ShapeDtypeStruct((TILE, LANES), jnp.float32),
        ],
        compiler_params=pltpu.CompilerParams(dimension_semantics=("arbitrary",)),
        cost_estimate=pl.CostEstimate(flops=work * COST, transcendentals=0, bytes_accessed=work * SEG * 4),
        name="spectrum",
    )(
        by_channel(x),
        by_channel(remote),
        by_channel(halo),
        reals,
        left,
        second,
        edges,
    )


def gather_kernel(tiles, first, x_hbm, halo_out, swap_out, halo_buf, swap_buf, sems):
    core = lax.axis_index("tm") & 1
    mine = core * SIDE + first
    theirs = (1 - core) * SIDE + first
    edge = pl.multiple_of(core * (HALF * TILE), HALF * TILE)
    loads = []
    stores = []
    for u in range(tiles):
        source = x_hbm.at[mine + u, pl.ds(edge, HALF * TILE), :]
        loads.append(pltpu.make_async_copy(source, halo_buf.at[u], sems.at[0, u]))
        stores.append(pltpu.make_async_copy(halo_buf.at[u], halo_out.at[u], sems.at[1, u]))
    for u in range(tiles):
        loads.append(pltpu.make_async_copy(x_hbm.at[theirs + u], swap_buf.at[u], sems.at[0, tiles + u]))
        stores.append(pltpu.make_async_copy(swap_buf.at[u], swap_out.at[u], sems.at[1, tiles + u]))
    for copy in loads:
        copy.start()
    for load, store in zip(loads, stores):
        load.wait()
        store.start()
    for copy in stores:
        copy.wait()


def gather(tiles, first, x):
    hbm = pl.BlockSpec(memory_space=pl.ANY)
    return pl.pallas_call(
        functools.partial(gather_kernel, tiles, first),
        in_specs=[hbm],
        out_specs=[hbm, hbm],
        out_shape=[
            jax.ShapeDtypeStruct((tiles, HALF * TILE, LANES), jnp.float32),
            jax.ShapeDtypeStruct((tiles, ROOT * TILE, LANES), jnp.float32),
        ],
        scratch_shapes=[
            pltpu.VMEM((tiles, HALF * TILE, LANES), jnp.float32),
            pltpu.VMEM((tiles, ROOT * TILE, LANES), jnp.float32),
            pltpu.SemaphoreType.DMA((2, 2 * tiles)),
        ],
        name="gather",
    )(x)


def pick_constant():
    table = np.zeros((2, 2 * LANES, LANES), np.float32)
    for q in range(2):
        for k in range(HALF):
            table[q, q * HALF + k, k] = 1.0
            table[q, LANES + q * HALF + k, ROOT - k if k else HALF] = 1.0
    return table


def finish_kernel(scale_ref, pick_ref, *refs):
    parts, (power_ref, mean_ref, nyquist_ref, band, spread) = refs[:STEPS], refs[STEPS:]
    shard = lax.axis_index("tm")
    done = 0
    for tiles, part in zip(CHUNKS, parts):
        for core in range(2):
            total = part[core, : 2 * tiles]
            for source in range(2 + core, PLACES, 2):
                total = total + part[source, : 2 * tiles]
            first = (core * SIDE + done) * 2 * TILE
            band[first : first + 2 * tiles * TILE] = total.reshape(2 * tiles * TILE, LANES)
        done += tiles
    scale = scale_ref[0]
    lane = lax.broadcasted_iota(jnp.int32, (1, LANES), 1)
    sums = []
    for k in range(2):
        count = band.shape[0] // 4
        lo = band[pl.ds(2 * k, count, stride=4), :]
        hi = band[pl.ds(2 * k + 1, count, stride=4), :]
        both = jnp.concatenate([lo, hi], axis=1)
        first = (lane == 0) & (shard == 0) & (k == 0)
        factor = jnp.where(first, scale, 2.0 * scale)
        total = jnp.zeros((1, LANES), jnp.float32)
        for q in range(2):
            value = (
                jnp.dot(both, pick_ref[q], preferred_element_type=jnp.float32, precision=lax.Precision.HIGHEST)
                * factor
            )
            spread[k, pl.ds(q, count, stride=2), :] = value
            total = total + jnp.sum(value, axis=0, keepdims=True)
        power_ref[:, k * LANES : (k + 1) * LANES] = spread[k]
        sums.append(total)
    mean_ref[...] = jnp.concatenate(sums, axis=1)
    for core in range(2):
        total = parts[-1][core, 2 * CHUNKS[-1]]
        for source in range(2 + core, PLACES, 2):
            total = total + parts[-1][source, 2 * CHUNKS[-1]]
        nyquist_ref[core * SIDE : (core + 1) * SIDE] = (total * scale).T[:SIDE]


def finish(scale, parts, rows):
    vmem = pl.BlockSpec(memory_space=pltpu.VMEM)
    smem = pl.BlockSpec(memory_space=pltpu.SMEM)
    return pl.pallas_call(
        finish_kernel,
        in_specs=[smem, vmem] + [vmem] * len(parts),
        out_specs=[vmem, vmem, vmem],
        out_shape=[
            jax.ShapeDtypeStruct((rows, 2 * LANES), jnp.float32),
            jax.ShapeDtypeStruct((1, 2 * LANES), jnp.float32),
            jax.ShapeDtypeStruct((2 * SIDE, TILE), jnp.float32),
        ],
        scratch_shapes=[
            pltpu.VMEM((rows * 2, LANES), jnp.float32),
            pltpu.VMEM((2, rows, LANES), jnp.float32),
        ],
        name="finish",
    )(scale, pick_constant(), *parts)


def per_device(strain):
    rows, width = strain.shape
    count = lax.axis_size("tm")
    row_tiles = rows // TILE
    segments = width // (SEG // 2) * count - 1
    x = strain.reshape(row_tiles, TILE, ROOT, LANES).swapaxes(1, 2).reshape(row_tiles, ROOT * TILE, LANES)
    same = [(i + 2, i) for i in range(0, count - 2, 2)] + [(i, i + 2) for i in range(1, count - 2, 2)]
    swap = [(i, i ^ 1) for i in range(count)]

    moved = []
    for at, tiles in ((0, CHUNKS[0]), (CHUNKS[0], SIDE - CHUNKS[0])):
        edge, other = gather(tiles, at, x)
        halo = lax.ppermute(edge, "tm", same)
        remote = lax.ppermute(other, "tm", swap)
        moved.append((remote, halo))
    constants = dft_constants()
    scale = jnp.full((1,), 1.0 / (segments * constants[3]), jnp.float32)
    edges = np.zeros((TILE, LANES), np.float32)
    parts = []
    done = 0
    for step, tiles in enumerate(CHUNKS):
        out, edges = spectrum(
            done,
            tiles,
            done - CHUNKS[0] if step else 0,
            step == STEPS - 1,
            x,
            *moved[min(step, 1)],
            constants,
            edges,
        )
        parts.append(lax.all_to_all(out, "tm", 0, 0, tiled=True))
        done += tiles
    power, band_sum, nyquist = finish(scale, parts, rows)
    chans = lax.axis_size("chan")
    total = band_sum
    for shift in range(1, chans):
        total = total + lax.ppermute(band_sum, "chan", [(i, (i + shift) % chans) for i in range(chans)])
    mean_power = (total / (rows * chans)).reshape(-1)
    return power, nyquist.reshape(-1), mean_power


def solution(mesh):
    in_specs = (P("chan", "tm"),)
    out_specs = (P("chan", "tm"), P("chan"), P("tm"))
    return jax.shard_map(per_device, mesh=mesh, in_specs=in_specs, out_specs=out_specs, check_vma=False)
```

```python
import functools

import jax
import jax.numpy as jnp
import numpy as np
from jax import lax
from jax.experimental import pallas as pl
from jax.experimental.pallas import tpu as pltpu
from jax.sharding import PartitionSpec as P


SEG = 16384
ROOT = 128
HALF = ROOT // 2
TILE = 8
LANES = 128
CHUNKS = (5, 7)
STEPS = len(CHUNKS)
SIDE = 12
PLACES = 32
SEGS = 4
COST = 1 << 22


def split_bf16(table):
    high = table.astype(jnp.bfloat16)
    low = (table - high.astype(np.float64)).astype(jnp.bfloat16)
    return high, low


def dft_constants():
    n = np.arange(ROOT)
    angle = 2.0 * np.pi * ((n[:, None] * n[None, :]) % ROOT) / ROOT
    rows = np.arange(HALF)
    first = np.concatenate([np.cos(angle[:HALF]), -np.sin(angle[:HALF])], axis=0)
    first[HALF] = 1.0 - 2.0 * (n % 2)
    high, low = split_bf16(first)
    first_high = np.concatenate([high, high], axis=1)
    twist = 2.0 * np.pi * (rows[:, None] * n[None, :]) / SEG
    cos_twist = np.cos(twist)
    cos_imag = cos_twist.copy()
    cos_imag[0] = 0.0
    twiddle = np.stack([cos_twist, cos_imag, np.sin(twist)]).astype(np.float32)
    edge = np.pi * n / ROOT
    edge_twiddle = np.stack([np.cos(edge), -np.sin(edge)]).astype(np.float32)
    columns = []
    for k in range(HALF):
        columns += [k, ROOT - 1 - k]
    c = np.cos(angle[:, columns])
    s = np.sin(angle[:, columns])
    high, low_second = split_bf16(np.block([[c, -s], [s, c]]))
    second = np.concatenate([high, high, low_second], axis=0)
    window = (0.5 - 0.5 * np.cos(2.0 * np.pi * np.arange(SEG) / SEG)).astype(np.float32)
    reals = np.concatenate([window.reshape(ROOT, LANES), *twiddle, edge_twiddle, np.zeros((6, LANES), np.float32)])
    left = np.concatenate([first_high, low], axis=1)
    return reals, left, second, float(np.sum(window.astype(np.float64) ** 2))


def spectrum_kernel(
    tiles,
    first,
    skip,
    last,
    x_hbm,
    remote_hbm,
    halo_hbm,
    reals_ref,
    first_ref,
    second_ref,
    edges_in_ref,
    out_ref,
    edges_ref,
    x_buf,
    means,
    spec,
    corner,
    result,
    sems,
):
    step = pl.program_id(0)
    me = lax.axis_index("tm")
    core = me & 1
    right = core
    near = pl.multiple_of(HALF + ROOT * core, HALF)
    far = pl.multiple_of(HALF + ROOT * (1 - core), HALF)
    outer_at = pl.multiple_of(right * (5 * HALF), HALF)
    outer_start = pl.multiple_of(right * (4 * HALF), HALF)
    starts = (HALF, 2 * HALF, 3 * HALF, outer_start)
    inside = jnp.where(right == 1, me < lax.axis_size("tm") - 2, me > 1)
    keep = jnp.where(inside, 1.0, 0.0).astype(jnp.float32)
    base = step

    def load(u):
        for c in range(TILE):
            for src, at, size in (
                (x_hbm.at[core * SIDE + first + u, :, c, 0, :], near, ROOT),
                (remote_hbm.at[skip + u, :, c, 0, :], far, ROOT),
                (halo_hbm.at[skip + u, :, c, 0, :], outer_at, HALF),
            ):
                pltpu.make_async_copy(src, x_buf.at[u, c, pl.ds(at, size), :], sems.at[u]).start()

    @pl.when(step == 0)
    def _():
        load(0)
        if tiles > 1:
            load(1)
        edges_ref[...] = edges_in_ref[...] if first else jnp.zeros((TILE, LANES), jnp.float32)

    @pl.when(step + 2 < tiles)
    def _():
        load(step + 2)

    def wait_for(u):
        whole = x_buf.at[base + u, :, pl.ds(0, 5 * HALF), :]
        pltpu.make_async_copy(whole, whole, sems.at[base + u]).wait()

    def average(u):
        def part(c, at):
            return jnp.sum(x_buf[base + u, c, pl.ds(at, HALF), :].reshape(HALF // TILE, TILE, LANES), axis=0)

        sums = [[] for _ in range(SEGS)]
        for c in range(TILE):
            q = [part(c, HALF * (k + 1)) for k in range(4)]
            outer = part(c, outer_at) + jnp.where(right == 1, q[3], q[0])
            for k, value in enumerate((q[0] + q[1], q[1] + q[2], q[2] + q[3], outer)):
                sums[k].append(value)
        both = jnp.stack(sum(sums, []))
        total = jnp.sum(jnp.sum(both, axis=1), axis=1, keepdims=True) * (1.0 / SEG)
        means[...] = jnp.broadcast_to(total, (SEGS * TILE, LANES))

    def put(pair, row, size, part, value):
        high = value.astype(jnp.bfloat16)
        lanes = slice(part * LANES, (part + 1) * LANES)
        lanes_low = slice((2 + part) * LANES, (3 + part) * LANES)
        spec[pair, row : row + size, lanes] = high
        spec[pair, row : row + size, lanes_low] = (value - high.astype(jnp.float32)).astype(jnp.bfloat16)

    rows = 2 * SEGS * HALF

    def forward(pair):
        for seg in range(SEGS):
            highs = []
            lows = []
            for q in range(2):
                c = 2 * pair + q
                r = seg * TILE + c
                piece = x_buf[step, c, pl.ds(starts[seg], ROOT), :]
                centred = (piece - means[r : r + 1, :]) * reals_ref[:ROOT]
                high = centred.astype(jnp.bfloat16)
                highs.append(high)
                lows.append((centred - high.astype(jnp.float32)).astype(jnp.bfloat16))
            high = jnp.concatenate(highs, axis=1)
            low = jnp.concatenate(lows, axis=1)
            stage = jnp.dot(
                first_ref[...], jnp.concatenate([high, low, high], axis=0), preferred_element_type=jnp.float32
            )
            for q in range(2):
                real = stage[:HALF, q * LANES : (q + 1) * LANES]
                imag = stage[HALF:, q * LANES : (q + 1) * LANES]
                r = 2 * seg + q
                corner[pair, r : r + 1, :] = imag[0:1]
                cos_real = reals_ref[ROOT : ROOT + HALF]
                cos_imag = reals_ref[ROOT + HALF : 2 * ROOT]
                sin_both = reals_ref[2 * ROOT : 2 * ROOT + HALF]
                put(pair, r * HALF, HALF, 0, real * cos_real + imag * sin_both)
                put(pair, r * HALF, HALF, 1, imag * cos_imag - real * sin_both)

    def second(pair):
        edge = 2 * ROOT + HALF
        for part in range(2):
            put(pair, rows, TILE, part, corner[pair] * reals_ref[edge + part : edge + part + 1])
        left = jnp.concatenate([spec[pair], spec[pair, :, : 2 * LANES]], axis=1)
        result[pair] = jnp.dot(left, second_ref[...], preferred_element_type=jnp.float32)

    row_id = lax.broadcasted_iota(jnp.int32, (HALF, LANES), 0)
    lane_id = lax.broadcasted_iota(jnp.int32, (HALF, LANES), 1)
    replaced = (row_id == 0) & (lane_id % 2 == 1)
    tile_lane = lax.broadcasted_iota(jnp.int32, (TILE, LANES), 1)
    tile_row = lax.broadcasted_iota(jnp.int32, (TILE, LANES), 0)
    lower_rows = tile_row < TILE // 2
    edge_rows = []

    def column(pair):
        def power_of(start, size):
            real = result[pair, start : start + size, :LANES]
            imag = result[pair, start : start + size, LANES:]
            return real * real + imag * imag

        edge_power = power_of(rows, TILE)
        blocks = []
        for q in range(2):
            total = keep * power_of((6 + q) * HALF, HALF)
            edge = keep * edge_power[6 + q : 7 + q]
            for seg in range(3):
                total = total + power_of((2 * seg + q) * HALF, HALF)
                edge = edge + edge_power[2 * seg + q : 2 * seg + q + 1]
            edge_rows.append(total[0:1])
            blocks.append(jnp.where(replaced, edge, total))
        return jnp.concatenate(blocks, axis=0).T

    def store(half, a, b):
        at = 2 * step + half
        for place in range(PLACES // 2):
            va = a[place * TILE : (place + 1) * TILE]
            vb = b[place * TILE : (place + 1) * TILE]
            out_ref[2 * place, at] = jnp.where(lower_rows, va, pltpu.roll(vb, 4, 0))
            out_ref[2 * place + 1, at] = jnp.where(lower_rows, pltpu.roll(va, 4, 0), vb)

    wait_for(0)
    average(0)
    forward(0)
    second(0)
    forward(1)
    second(1)
    first_column = column(0)
    forward(2)
    second(2)
    store(0, first_column, column(1))
    forward(3)
    second(3)
    first_column = column(2)
    store(1, first_column, column(3))
    edge_tile = jnp.zeros((TILE, LANES), jnp.float32)
    for c, row in enumerate(edge_rows):
        edge_tile = jnp.where(tile_row == c, row, edge_tile)
    edge_value = jnp.sum(jnp.where(tile_lane == LANES - 1, edge_tile, 0.0), axis=1, keepdims=True)
    edges_ref[...] = jnp.where(tile_lane == first + step, edge_value, edges_ref[...])
    if last:

        @pl.when(step == tiles - 1)
        def _():
            for place in range(PLACES):
                out_ref[place, 2 * tiles] = edges_ref[...]


def spectrum(first, tiles, skip, last, x, remote, halo, constants, edges):
    reals, left, second, _ = constants
    whole = lambda shape: pl.BlockSpec(shape, lambda i: (0,) * len(shape))
    hbm = pl.BlockSpec(memory_space=pl.ANY)
    out_shape = (PLACES, 2 * tiles + int(last), TILE, LANES)
    rows = 2 * SEGS * HALF + TILE
    by_channel = lambda v: v.reshape(-1, v.shape[1] // TILE, TILE, 1, LANES)
    work = tiles * SEGS * TILE
    return pl.pallas_call(
        functools.partial(spectrum_kernel, tiles, first, skip, last),
        grid_spec=pltpu.PrefetchScalarGridSpec(
            num_scalar_prefetch=0,
            grid=(tiles,),
            in_specs=[
                hbm,
                hbm,
                hbm,
                whole(reals.shape),
                whole(left.shape),
                whole(second.shape),
                whole((TILE, LANES)),
            ],
            out_specs=[whole(out_shape), whole((TILE, LANES))],
            scratch_shapes=[
                pltpu.VMEM((tiles, TILE, 6 * HALF, LANES), jnp.float32),
                pltpu.VMEM((SEGS * TILE, LANES), jnp.float32),
                pltpu.VMEM((TILE // 2, rows, 4 * LANES), jnp.bfloat16),
                pltpu.VMEM((TILE // 2, TILE, LANES), jnp.float32),
                pltpu.VMEM((TILE // 2, rows, 2 * LANES), jnp.float32),
                pltpu.SemaphoreType.DMA((tiles,)),
            ],
        ),
        out_shape=[
            jax.ShapeDtypeStruct(out_shape, jnp.float32),
            jax.ShapeDtypeStruct((TILE, LANES), jnp.float32),
        ],
        compiler_params=pltpu.CompilerParams(dimension_semantics=("arbitrary",)),
        cost_estimate=pl.CostEstimate(flops=work * COST, transcendentals=0, bytes_accessed=work * SEG * 4),
        name="spectrum",
    )(
        by_channel(x),
        by_channel(remote),
        by_channel(halo),
        reals,
        left,
        second,
        edges,
    )


def gather_kernel(tiles, first, x_hbm, halo_out, swap_out, halo_buf, swap_buf, sems):
    core = lax.axis_index("tm") & 1
    theirs = (1 - core) * SIDE + first
    edge = pl.multiple_of(core * (HALF * TILE), HALF * TILE)
    loads = []
    stores = []
    for u in range(tiles):
        source = x_hbm.at[theirs + u, pl.ds(edge, HALF * TILE), :]
        loads.append(pltpu.make_async_copy(source, halo_buf.at[u], sems.at[0, u]))
        stores.append(pltpu.make_async_copy(halo_buf.at[u], halo_out.at[u], sems.at[1, u]))
    for u in range(tiles):
        loads.append(pltpu.make_async_copy(x_hbm.at[theirs + u], swap_buf.at[u], sems.at[0, tiles + u]))
        stores.append(pltpu.make_async_copy(swap_buf.at[u], swap_out.at[u], sems.at[1, tiles + u]))
    for copy in loads:
        copy.start()
    for load, store in zip(loads, stores):
        load.wait()
        store.start()
    for copy in stores:
        copy.wait()


def gather(tiles, first, x):
    hbm = pl.BlockSpec(memory_space=pl.ANY)
    return pl.pallas_call(
        functools.partial(gather_kernel, tiles, first),
        in_specs=[hbm],
        out_specs=[hbm, hbm],
        out_shape=[
            jax.ShapeDtypeStruct((tiles, HALF * TILE, LANES), jnp.float32),
            jax.ShapeDtypeStruct((tiles, ROOT * TILE, LANES), jnp.float32),
        ],
        scratch_shapes=[
            pltpu.VMEM((tiles, HALF * TILE, LANES), jnp.float32),
            pltpu.VMEM((tiles, ROOT * TILE, LANES), jnp.float32),
            pltpu.SemaphoreType.DMA((2, 2 * tiles)),
        ],
        name="gather",
    )(x)


def pick_constant():
    table = np.zeros((2, 2 * LANES, LANES), np.float32)
    for q in range(2):
        for k in range(HALF):
            table[q, q * HALF + k, k] = 1.0
            table[q, LANES + q * HALF + k, ROOT - k if k else HALF] = 1.0
    return table


def finish_kernel(scale_ref, pick_ref, *refs):
    parts, (power_ref, mean_ref, nyquist_ref, band, spread) = refs[:STEPS], refs[STEPS:]
    shard = lax.axis_index("tm")
    done = 0
    for tiles, part in zip(CHUNKS, parts):
        for core in range(2):
            total = part[core, : 2 * tiles]
            for source in range(2 + core, PLACES, 2):
                total = total + part[source, : 2 * tiles]
            first = (core * SIDE + done) * 2 * TILE
            band[first : first + 2 * tiles * TILE] = total.reshape(2 * tiles * TILE, LANES)
        done += tiles
    scale = scale_ref[0]
    lane = lax.broadcasted_iota(jnp.int32, (1, LANES), 1)
    sums = []
    for k in range(2):
        count = band.shape[0] // 4
        lo = band[pl.ds(2 * k, count, stride=4), :]
        hi = band[pl.ds(2 * k + 1, count, stride=4), :]
        both = jnp.concatenate([lo, hi], axis=1)
        first = (lane == 0) & (shard == 0) & (k == 0)
        factor = jnp.where(first, scale, 2.0 * scale)
        total = jnp.zeros((1, LANES), jnp.float32)
        for q in range(2):
            value = (
                jnp.dot(both, pick_ref[q], preferred_element_type=jnp.float32, precision=lax.Precision.HIGHEST)
                * factor
            )
            spread[k, pl.ds(q, count, stride=2), :] = value
            total = total + jnp.sum(value, axis=0, keepdims=True)
        power_ref[:, k * LANES : (k + 1) * LANES] = spread[k]
        sums.append(total)
    mean_ref[...] = jnp.concatenate(sums, axis=1)
    for core in range(2):
        total = parts[-1][core, 2 * CHUNKS[-1]]
        for source in range(2 + core, PLACES, 2):
            total = total + parts[-1][source, 2 * CHUNKS[-1]]
        nyquist_ref[core * SIDE : (core + 1) * SIDE] = (total * scale).T[:SIDE]


def finish(scale, parts, rows):
    vmem = pl.BlockSpec(memory_space=pltpu.VMEM)
    smem = pl.BlockSpec(memory_space=pltpu.SMEM)
    return pl.pallas_call(
        finish_kernel,
        in_specs=[smem, vmem] + [vmem] * len(parts),
        out_specs=[vmem, vmem, vmem],
        out_shape=[
            jax.ShapeDtypeStruct((rows, 2 * LANES), jnp.float32),
            jax.ShapeDtypeStruct((1, 2 * LANES), jnp.float32),
            jax.ShapeDtypeStruct((2 * SIDE, TILE), jnp.float32),
        ],
        scratch_shapes=[
            pltpu.VMEM((rows * 2, LANES), jnp.float32),
            pltpu.VMEM((2, rows, LANES), jnp.float32),
        ],
        name="finish",
    )(scale, pick_constant(), *parts)


def per_device(strain):
    rows, width = strain.shape
    count = lax.axis_size("tm")
    row_tiles = rows // TILE
    segments = width // (SEG // 2) * count - 1
    x = strain.reshape(row_tiles, TILE, ROOT, LANES).swapaxes(1, 2).reshape(row_tiles, ROOT * TILE, LANES)
    cross = [(i, i + 1) for i in range(1, count - 2, 2)] + [(i + 1, i) for i in range(1, count - 2, 2)]
    swap = [(i, i ^ 1) for i in range(count)]

    moved = []
    for at, tiles in ((0, CHUNKS[0]), (CHUNKS[0], SIDE - CHUNKS[0])):
        edge, other = gather(tiles, at, x)
        halo = lax.ppermute(edge, "tm", cross)
        remote = lax.ppermute(other, "tm", swap)
        moved.append((remote, halo))
    constants = dft_constants()
    scale = jnp.full((1,), 1.0 / (segments * constants[3]), jnp.float32)
    edges = np.zeros((TILE, LANES), np.float32)
    parts = []
    done = 0
    for step, tiles in enumerate(CHUNKS):
        out, edges = spectrum(
            done,
            tiles,
            done - CHUNKS[0] if step else 0,
            step == STEPS - 1,
            x,
            *moved[min(step, 1)],
            constants,
            edges,
        )
        parts.append(lax.all_to_all(out, "tm", 0, 0, tiled=True))
        done += tiles
    power, band_sum, nyquist = finish(scale, parts, rows)
    chans = lax.axis_size("chan")
    total = band_sum
    for shift in range(1, chans):
        total = total + lax.ppermute(band_sum, "chan", [(i, (i + shift) % chans) for i in range(chans)])
    mean_power = (total / (rows * chans)).reshape(-1)
    return power, nyquist.reshape(-1), mean_power


def solution(mesh):
    in_specs = (P("chan", "tm"),)
    out_specs = (P("chan", "tm"), P("chan"), P("tm"))
    return jax.shard_map(per_device, mesh=mesh, in_specs=in_specs, out_specs=out_specs, check_vma=False)
```

```python
import functools

import jax
import jax.numpy as jnp
import numpy as np
from jax import lax
from jax.experimental import pallas as pl
from jax.experimental.pallas import tpu as pltpu
from jax.sharding import PartitionSpec as P


SEG = 16384
ROOT = 128
HALF = ROOT // 2
TILE = 8
LANES = 128
CHUNKS = (5, 7)
STEPS = len(CHUNKS)
SIDE = 12
PLACES = 32
SEGS = 4
COST = 1 << 22


def split_bf16(table):
    high = table.astype(jnp.bfloat16)
    low = (table - high.astype(np.float64)).astype(jnp.bfloat16)
    return high, low


def dft_constants():
    n = np.arange(ROOT)
    angle = 2.0 * np.pi * ((n[:, None] * n[None, :]) % ROOT) / ROOT
    rows = np.arange(HALF)
    first = np.concatenate([np.cos(angle[:HALF]), -np.sin(angle[:HALF])], axis=0)
    first[HALF] = 1.0 - 2.0 * (n % 2)
    high, low = split_bf16(first)
    first_high = np.concatenate([high, high], axis=1)
    twist = 2.0 * np.pi * (rows[:, None] * n[None, :]) / SEG
    cos_twist = np.cos(twist)
    cos_imag = cos_twist.copy()
    cos_imag[0] = 0.0
    twiddle = np.stack([cos_twist, cos_imag, np.sin(twist)]).astype(np.float32)
    edge = np.pi * n / ROOT
    edge_twiddle = np.stack([np.cos(edge), -np.sin(edge)]).astype(np.float32)
    columns = []
    for k in range(HALF):
        columns += [k, ROOT - 1 - k]
    c = np.cos(angle[:, columns])
    s = np.sin(angle[:, columns])
    high, low_second = split_bf16(np.block([[c, -s], [s, c]]))
    second = np.concatenate([high, high, low_second], axis=0)
    window = (0.5 - 0.5 * np.cos(2.0 * np.pi * np.arange(SEG) / SEG)).astype(np.float32)
    reals = np.concatenate([window.reshape(ROOT, LANES), *twiddle, edge_twiddle, np.zeros((6, LANES), np.float32)])
    left = np.concatenate([first_high, low], axis=1)
    return reals, left, second, float(np.sum(window.astype(np.float64) ** 2))


def spectrum_kernel(
    tiles,
    first,
    skip,
    last,
    x_hbm,
    remote_hbm,
    halo_hbm,
    reals_ref,
    first_ref,
    second_ref,
    edges_in_ref,
    out_ref,
    edges_ref,
    x_buf,
    means,
    spec,
    corner,
    result,
    sems,
):
    step = pl.program_id(0)
    me = lax.axis_index("tm")
    core = me & 1
    right = core
    near = pl.multiple_of(HALF + ROOT * core, HALF)
    far = pl.multiple_of(HALF + ROOT * (1 - core), HALF)
    outer_at = pl.multiple_of(right * (5 * HALF), HALF)
    outer_start = pl.multiple_of(right * (4 * HALF), HALF)
    starts = (HALF, 2 * HALF, 3 * HALF, outer_start)
    inside = jnp.where(right == 1, me < lax.axis_size("tm") - 2, me > 1)
    keep = jnp.where(inside, 1.0, 0.0).astype(jnp.float32)
    base = step

    def load(u):
        for c in range(TILE):
            for src, at, size in (
                (x_hbm.at[core * SIDE + first + u, :, c, 0, :], near, ROOT),
                (remote_hbm.at[skip + u, :, c, 0, :], far, ROOT),
                (halo_hbm.at[skip + u, :, c, 0, :], outer_at, HALF),
            ):
                pltpu.make_async_copy(src, x_buf.at[u, c, pl.ds(at, size), :], sems.at[u]).start()

    @pl.when(step == 0)
    def _():
        load(0)
        if tiles > 1:
            load(1)
        edges_ref[...] = edges_in_ref[...] if first else jnp.zeros((TILE, LANES), jnp.float32)

    @pl.when(step + 2 < tiles)
    def _():
        load(step + 2)

    def wait_for(u):
        whole = x_buf.at[base + u, :, pl.ds(0, 5 * HALF), :]
        pltpu.make_async_copy(whole, whole, sems.at[base + u]).wait()

    def average(u):
        def part(c, at):
            return jnp.sum(x_buf[base + u, c, pl.ds(at, HALF), :].reshape(HALF // TILE, TILE, LANES), axis=0)

        sums = [[] for _ in range(SEGS)]
        for c in range(TILE):
            q = [part(c, HALF * (k + 1)) for k in range(4)]
            outer = part(c, outer_at) + jnp.where(right == 1, q[3], q[0])
            for k, value in enumerate((q[0] + q[1], q[1] + q[2], q[2] + q[3], outer)):
                sums[k].append(value)
        both = jnp.stack(sum(sums, []))
        total = jnp.sum(jnp.sum(both, axis=1), axis=1, keepdims=True) * (1.0 / SEG)
        means[...] = jnp.broadcast_to(total, (SEGS * TILE, LANES))

    def put(pair, row, size, part, value):
        high = value.astype(jnp.bfloat16)
        lanes = slice(part * LANES, (part + 1) * LANES)
        lanes_low = slice((2 + part) * LANES, (3 + part) * LANES)
        spec[pair, row : row + size, lanes] = high
        spec[pair, row : row + size, lanes_low] = (value - high.astype(jnp.float32)).astype(jnp.bfloat16)

    rows = 2 * SEGS * HALF

    def forward(pair):
        for seg in range(SEGS):
            highs = []
            lows = []
            for q in range(2):
                c = 2 * pair + q
                r = seg * TILE + c
                piece = x_buf[step, c, pl.ds(starts[seg], ROOT), :]
                centred = (piece - means[r : r + 1, :]) * reals_ref[:ROOT]
                high = centred.astype(jnp.bfloat16)
                highs.append(high)
                lows.append((centred - high.astype(jnp.float32)).astype(jnp.bfloat16))
            high = jnp.concatenate(highs, axis=1)
            low = jnp.concatenate(lows, axis=1)
            stage = jnp.dot(
                first_ref[...], jnp.concatenate([high, low, high], axis=0), preferred_element_type=jnp.float32
            )
            for q in range(2):
                real = stage[:HALF, q * LANES : (q + 1) * LANES]
                imag = stage[HALF:, q * LANES : (q + 1) * LANES]
                r = 2 * seg + q
                corner[pair, r : r + 1, :] = imag[0:1]
                cos_real = reals_ref[ROOT : ROOT + HALF]
                cos_imag = reals_ref[ROOT + HALF : 2 * ROOT]
                sin_both = reals_ref[2 * ROOT : 2 * ROOT + HALF]
                put(pair, r * HALF, HALF, 0, real * cos_real + imag * sin_both)
                put(pair, r * HALF, HALF, 1, imag * cos_imag - real * sin_both)

    def second(pair):
        edge = 2 * ROOT + HALF
        for part in range(2):
            put(pair, rows, TILE, part, corner[pair] * reals_ref[edge + part : edge + part + 1])
        left = jnp.concatenate([spec[pair], spec[pair, :, : 2 * LANES]], axis=1)
        result[pair] = jnp.dot(left, second_ref[...], preferred_element_type=jnp.float32)

    row_id = lax.broadcasted_iota(jnp.int32, (HALF, LANES), 0)
    lane_id = lax.broadcasted_iota(jnp.int32, (HALF, LANES), 1)
    replaced = (row_id == 0) & (lane_id % 2 == 1)
    tile_lane = lax.broadcasted_iota(jnp.int32, (TILE, LANES), 1)
    tile_row = lax.broadcasted_iota(jnp.int32, (TILE, LANES), 0)
    lower_rows = tile_row < TILE // 2
    edge_rows = []

    def column(pair):
        def power_of(start, size):
            real = result[pair, start : start + size, :LANES]
            imag = result[pair, start : start + size, LANES:]
            return real * real + imag * imag

        edge_power = power_of(rows, TILE)
        blocks = []
        for q in range(2):
            total = keep * power_of((6 + q) * HALF, HALF)
            edge = keep * edge_power[6 + q : 7 + q]
            for seg in range(3):
                total = total + power_of((2 * seg + q) * HALF, HALF)
                edge = edge + edge_power[2 * seg + q : 2 * seg + q + 1]
            edge_rows.append(total[0:1])
            blocks.append(jnp.where(replaced, edge, total))
        return jnp.concatenate(blocks, axis=0).T

    def store(half, a, b):
        at = 2 * step + half
        for place in range(PLACES // 2):
            va = a[place * TILE : (place + 1) * TILE]
            vb = b[place * TILE : (place + 1) * TILE]
            out_ref[2 * place, at] = jnp.where(lower_rows, va, pltpu.roll(vb, 4, 0))
            out_ref[2 * place + 1, at] = jnp.where(lower_rows, pltpu.roll(va, 4, 0), vb)

    wait_for(0)
    average(0)
    forward(0)
    second(0)
    forward(1)
    second(1)
    first_column = column(0)
    forward(2)
    second(2)
    store(0, first_column, column(1))
    forward(3)
    second(3)
    first_column = column(2)
    store(1, first_column, column(3))
    edge_tile = jnp.zeros((TILE, LANES), jnp.float32)
    for c, row in enumerate(edge_rows):
        edge_tile = jnp.where(tile_row == c, row, edge_tile)
    edge_value = jnp.sum(jnp.where(tile_lane == LANES - 1, edge_tile, 0.0), axis=1, keepdims=True)
    edges_ref[...] = jnp.where(tile_lane == first + step, edge_value, edges_ref[...])
    if last:

        @pl.when(step == tiles - 1)
        def _():
            for place in range(PLACES):
                out_ref[place, 2 * tiles] = edges_ref[...]


def spectrum(first, tiles, skip, last, x, remote, halo, constants, edges):
    reals, left, second, _ = constants
    whole = lambda shape: pl.BlockSpec(shape, lambda i: (0,) * len(shape))
    hbm = pl.BlockSpec(memory_space=pl.ANY)
    out_shape = (PLACES, 2 * tiles + int(last), TILE, LANES)
    rows = 2 * SEGS * HALF + TILE
    by_channel = lambda v: v.reshape(-1, v.shape[1] // TILE, TILE, 1, LANES)
    work = tiles * SEGS * TILE
    return pl.pallas_call(
        functools.partial(spectrum_kernel, tiles, first, skip, last),
        grid_spec=pltpu.PrefetchScalarGridSpec(
            num_scalar_prefetch=0,
            grid=(tiles,),
            in_specs=[
                hbm,
                hbm,
                hbm,
                whole(reals.shape),
                whole(left.shape),
                whole(second.shape),
                whole((TILE, LANES)),
            ],
            out_specs=[whole(out_shape), whole((TILE, LANES))],
            scratch_shapes=[
                pltpu.VMEM((tiles, TILE, 6 * HALF, LANES), jnp.float32),
                pltpu.VMEM((SEGS * TILE, LANES), jnp.float32),
                pltpu.VMEM((TILE // 2, rows, 4 * LANES), jnp.bfloat16),
                pltpu.VMEM((TILE // 2, TILE, LANES), jnp.float32),
                pltpu.VMEM((TILE // 2, rows, 2 * LANES), jnp.float32),
                pltpu.SemaphoreType.DMA((tiles,)),
            ],
        ),
        out_shape=[
            jax.ShapeDtypeStruct(out_shape, jnp.float32),
            jax.ShapeDtypeStruct((TILE, LANES), jnp.float32),
        ],
        compiler_params=pltpu.CompilerParams(dimension_semantics=("arbitrary",)),
        cost_estimate=pl.CostEstimate(flops=work * COST, transcendentals=0, bytes_accessed=work * SEG * 4),
        name="spectrum",
    )(
        by_channel(x),
        by_channel(remote),
        by_channel(halo),
        reals,
        left,
        second,
        edges,
    )


def gather_kernel(tiles, first, kinds, x_hbm, *refs):
    outs, buffers, sems = refs[: len(kinds)], refs[len(kinds) : -1], refs[-1]
    core = lax.axis_index("tm") & 1
    theirs = (1 - core) * SIDE + first
    edge = pl.multiple_of(core * (HALF * TILE), HALF * TILE)
    loads = []
    stores = []
    for n, kind in enumerate(kinds):
        for u in range(tiles):
            source = x_hbm.at[theirs + u] if kind else x_hbm.at[theirs + u, pl.ds(edge, HALF * TILE), :]
            loads.append(pltpu.make_async_copy(source, buffers[n].at[u], sems.at[0, n * tiles + u]))
            stores.append(pltpu.make_async_copy(buffers[n].at[u], outs[n].at[u], sems.at[1, n * tiles + u]))
    for copy in loads:
        copy.start()
    for load, store in zip(loads, stores):
        load.wait()
        store.start()
    for copy in stores:
        copy.wait()


def gather(tiles, first, x, only=None):
    hbm = pl.BlockSpec(memory_space=pl.ANY)
    kinds = (0, 1) if only is None else (only,)
    shapes = [(tiles, (ROOT if kind else HALF) * TILE, LANES) for kind in kinds]
    out = pl.pallas_call(
        functools.partial(gather_kernel, tiles, first, kinds),
        in_specs=[hbm],
        out_specs=[hbm] * len(kinds),
        out_shape=[jax.ShapeDtypeStruct(shape, jnp.float32) for shape in shapes],
        scratch_shapes=[pltpu.VMEM(shape, jnp.float32) for shape in shapes]
        + [pltpu.SemaphoreType.DMA((2, len(kinds) * tiles))],
        name="gather",
    )(x)
    return out if only is None else out[0]


def pick_constant():
    table = np.zeros((2, 2 * LANES, LANES), np.float32)
    for q in range(2):
        for k in range(HALF):
            table[q, q * HALF + k, k] = 1.0
            table[q, LANES + q * HALF + k, ROOT - k if k else HALF] = 1.0
    return table


def finish_kernel(scale_ref, pick_ref, *refs):
    parts, (power_ref, mean_ref, nyquist_ref, band, spread) = refs[:STEPS], refs[STEPS:]
    shard = lax.axis_index("tm")
    done = 0
    for tiles, part in zip(CHUNKS, parts):
        for core in range(2):
            total = part[core, : 2 * tiles]
            for source in range(2 + core, PLACES, 2):
                total = total + part[source, : 2 * tiles]
            first = (core * SIDE + done) * 2 * TILE
            band[first : first + 2 * tiles * TILE] = total.reshape(2 * tiles * TILE, LANES)
        done += tiles
    scale = scale_ref[0]
    lane = lax.broadcasted_iota(jnp.int32, (1, LANES), 1)
    sums = []
    for k in range(2):
        count = band.shape[0] // 4
        lo = band[pl.ds(2 * k, count, stride=4), :]
        hi = band[pl.ds(2 * k + 1, count, stride=4), :]
        both = jnp.concatenate([lo, hi], axis=1)
        first = (lane == 0) & (shard == 0) & (k == 0)
        factor = jnp.where(first, scale, 2.0 * scale)
        total = jnp.zeros((1, LANES), jnp.float32)
        for q in range(2):
            value = (
                jnp.dot(both, pick_ref[q], preferred_element_type=jnp.float32, precision=lax.Precision.HIGHEST)
                * factor
            )
            spread[k, pl.ds(q, count, stride=2), :] = value
            total = total + jnp.sum(value, axis=0, keepdims=True)
        power_ref[:, k * LANES : (k + 1) * LANES] = spread[k]
        sums.append(total)
    mean_ref[...] = jnp.concatenate(sums, axis=1)
    for core in range(2):
        total = parts[-1][core, 2 * CHUNKS[-1]]
        for source in range(2 + core, PLACES, 2):
            total = total + parts[-1][source, 2 * CHUNKS[-1]]
        nyquist_ref[core * SIDE : (core + 1) * SIDE] = (total * scale).T[:SIDE]


def finish(scale, parts, rows):
    vmem = pl.BlockSpec(memory_space=pltpu.VMEM)
    smem = pl.BlockSpec(memory_space=pltpu.SMEM)
    return pl.pallas_call(
        finish_kernel,
        in_specs=[smem, vmem] + [vmem] * len(parts),
        out_specs=[vmem, vmem, vmem],
        out_shape=[
            jax.ShapeDtypeStruct((rows, 2 * LANES), jnp.float32),
            jax.ShapeDtypeStruct((1, 2 * LANES), jnp.float32),
            jax.ShapeDtypeStruct((2 * SIDE, TILE), jnp.float32),
        ],
        scratch_shapes=[
            pltpu.VMEM((rows * 2, LANES), jnp.float32),
            pltpu.VMEM((2, rows, LANES), jnp.float32),
        ],
        name="finish",
    )(scale, pick_constant(), *parts)


def per_device(strain):
    rows, width = strain.shape
    count = lax.axis_size("tm")
    row_tiles = rows // TILE
    segments = width // (SEG // 2) * count - 1
    x = strain.reshape(row_tiles, TILE, ROOT, LANES).swapaxes(1, 2).reshape(row_tiles, ROOT * TILE, LANES)
    cross = [(i, i + 1) for i in range(1, count - 2, 2)] + [(i + 1, i) for i in range(1, count - 2, 2)]
    swap = [(i, i ^ 1) for i in range(count)]

    moved = []
    for group, (at, tiles) in enumerate(((0, CHUNKS[0]), (CHUNKS[0], SIDE - CHUNKS[0]))):
        edge, other = gather(tiles, at, x) if group else (gather(tiles, at, x, 0), None)
        halo = lax.ppermute(edge, "tm", cross)
        if group == 0:
            other = gather(tiles, at, x, 1)
        remote = lax.ppermute(other, "tm", swap)
        moved.append((remote, halo))
    constants = dft_constants()
    scale = jnp.full((1,), 1.0 / (segments * constants[3]), jnp.float32)
    edges = constants[0]
    parts = []
    done = 0
    for step, tiles in enumerate(CHUNKS):
        out, edges = spectrum(
            done,
            tiles,
            done - CHUNKS[0] if step else 0,
            step == STEPS - 1,
            x,
            *moved[min(step, 1)],
            constants,
            edges,
        )
        parts.append(lax.all_to_all(out, "tm", 0, 0, tiled=True))
        done += tiles
    power, band_sum, nyquist = finish(scale, parts, rows)
    chans = lax.axis_size("chan")
    total = band_sum
    for shift in range(1, chans):
        total = total + lax.ppermute(band_sum, "chan", [(i, (i + shift) % chans) for i in range(chans)])
    mean_power = (total / (rows * chans)).reshape(-1)
    return power, nyquist.reshape(-1), mean_power


def solution(mesh):
    in_specs = (P("chan", "tm"),)
    out_specs = (P("chan", "tm"), P("chan"), P("tm"))
    return jax.shard_map(per_device, mesh=mesh, in_specs=in_specs, out_specs=out_specs, check_vma=False)
```
